16 devices in a mesh: dp: 1, sp: 16 (over x, y, z, core).
Axes of the slice: x: 2, y: 2, z: 2, core: 2. Of those that a mesh axis runs over, the one named last changes fastest.
Arguments:
- x: bfloat16 [4096, 4096], P(('dp', 'sp'))
- gain: bfloat16 [4096], replicated
- wq: bfloat16 [4096, 4096], replicated
- wk: bfloat16 [4096, 4096], replicated
- wv: bfloat16 [4096, 4096], replicated
- wo: bfloat16 [4096, 4096], replicated
Outputs:
- output: bfloat16 [4096, 4096], P(('dp', 'sp'))
All inputs are finite; a program needn't handle non-finite values.
Results may differ from the reference program's by a relative error of at most 0.012.
Values are sent between devices in bfloat16 or wider.
A program may use at most 2 GiB of HBM per device.

```python
import jax
import jax.numpy as jnp
from jax import lax

ROWS = 4096
D = 4096
HEADS = 16
KV_HEADS = 16
HEAD = 256
THETA = 10000


def setup_inputs(seed: int = 0, part: int = 0) -> dict:
    kx, kn, kq, kk, kv, ko = jax.random.split(jax.random.key(seed), 6)

    def weights(key, rows, columns):
        return jax.random.normal(key, (rows, columns), jnp.float32) * rows**-0.5

    drawn = {
        "x": jax.random.normal(jax.random.fold_in(kx, part), (ROWS, D), jnp.float32),
        "gain": 1 + 0.1 * jax.random.normal(kn, (D,), jnp.float32),
        "wq": 2 * weights(kq, D, HEADS * HEAD),
        "wk": 2 * weights(kk, D, KV_HEADS * HEAD),
        "wv": 4 * weights(kv, D, KV_HEADS * HEAD),
        "wo": weights(ko, HEADS * HEAD, D),
    }
    return {k: v.astype(jnp.bfloat16) for k, v in drawn.items()}


def normed(x, gain):
    wide = x.astype(jnp.float32)
    scale = lax.rsqrt(jnp.mean(wide * wide, -1, keepdims=True) + 1e-6)
    return (wide * scale * gain.astype(jnp.float32)).astype(jnp.bfloat16)


def turned(t, place, theta):
    half = t.shape[-1] // 2
    angle = place.astype(jnp.float32)[:, None] * theta ** (-jnp.arange(half, dtype=jnp.float32) / half)
    cos, sin = jnp.cos(angle)[:, None], jnp.sin(angle)[:, None]
    a, b = t[..., :half].astype(jnp.float32), t[..., half:].astype(jnp.float32)
    return jnp.concatenate([a * cos - b * sin, b * cos + a * sin], -1).astype(jnp.bfloat16)


def matmul(a, w):
    return jnp.dot(a, w, preferred_element_type=jnp.float32).astype(jnp.bfloat16)


def einsum(form, a, b):
    return jnp.einsum(form, a.astype(jnp.float32), b.astype(jnp.float32))


def attention(q, k, v):
    scores = einsum("tgsd,ugd->gstu", q, k) * q.shape[-1] ** -0.5
    token = jnp.arange(q.shape[0])
    scores = jnp.where(token[:, None] >= token, scores, -jnp.inf)
    weights = jax.nn.softmax(scores, -1).astype(jnp.bfloat16)
    return einsum("gstu,ugd->tgsd", weights, v).astype(jnp.bfloat16)


def reference(x, gain, wq, wk, wv, wo):
    a, place = normed(x, gain), jnp.arange(ROWS)
    q = turned(matmul(a, wq).reshape(ROWS, HEADS, HEAD), place, THETA).reshape(ROWS, KV_HEADS, -1, HEAD)
    k = turned(matmul(a, wk).reshape(ROWS, KV_HEADS, HEAD), place, THETA)
    v = matmul(a, wv).reshape(ROWS, KV_HEADS, HEAD)
    seen = attention(q, k, v).reshape(ROWS, HEADS * HEAD)
    return (x.astype(jnp.float32) + jnp.dot(seen, wo, preferred_element_type=jnp.float32)).astype(jnp.bfloat16)
```

```python
import functools

import jax
import jax.numpy as jnp
from jax import lax
from jax.experimental import pallas as pl
from jax.experimental.pallas import tpu as pltpu
from jax.sharding import PartitionSpec as P

HEAD = 256
THETA = 10000
LOG2E = 1.4426950408889634
HIDDEN = -2e30
MESH = pl.DeviceIdType.MESH
OWN = 256
PAIR = 2 * HEAD
CHIPS = 8
DIM = 4096
ONES = 16
AHEAD = 2

LINKS = [6, 1, 5, 2, 3, 4, 7]
SEND = [LINKS + [0], LINKS + [0], [0] + LINKS]
TAKE = [0] + LINKS


def digits(values):
    return sum(v * 8**i for i, v in enumerate(values))


def flipped(n, mask):
    out = n
    for b in range(3):
        bit = lax.rem(lax.div(n, 2**b), 2)
        flip = lax.rem(lax.div(mask, 2**b), 2)
        out = out + flip * (1 - 2 * bit) * 2**b
    return out


def dot(a, b, ca, cb):
    return lax.dot_general(a, b, (((ca,), (cb,)), ((), ())), preferred_element_type=jnp.float32)


def kernel(x_hbm, gain_ref, cos_ref, sin_ref, wq_hbm, wk_hbm, wv_hbm, wo_hbm, y_hbm,
           x_ref, a_ref, w_ref, wo_ref, out_ref, keys, values, queries, seen_out, seen_in, top_s, mix_s, acc_ref,
           x_sem, w_sem, wo_sem, y_sem, send_sem, recv_sem):
    me = lax.axis_index("sp")
    chip, core = lax.div(me, 2), lax.rem(me, 2)
    wide = [wk_hbm, wv_hbm, wq_hbm]

    def load_w(p, slot, other):
        return pltpu.make_async_copy(wide[p].at[:, pl.ds(pl.multiple_of(other * PAIR, PAIR), PAIR)], w_ref.at[slot], w_sem.at[slot])

    def load_wo(slot, other):
        return pltpu.make_async_copy(wo_hbm.at[pl.ds(pl.multiple_of(other * PAIR, PAIR), PAIR), :], wo_ref.at[slot], wo_sem.at[slot])

    def landing(p, c, b):
        at = pl.ds(pl.multiple_of(b * OWN, OWN), OWN)
        if p == 0:
            return keys.at[c, at, :]
        if p == 1:
            return values.at[c, pl.ds(0, HEAD), at]
        if p == 2:
            return queries.at[c, at, :]
        return seen_in.at[:, pl.ds(pl.multiple_of(c * PAIR + b * HEAD, HEAD), HEAD)]

    def part(p, i, b):
        if p < 3:
            return out_ref.at[p * CHIPS + i, b]
        return seen_out.at[i, pl.ds(b * OWN, OWN), :]

    def sending(p, i, b, to):
        return pltpu.make_async_remote_copy(
            src_ref=part(p, i, b), dst_ref=landing(p, chip, core), send_sem=send_sem.at[p, i, b],
            recv_sem=recv_sem.at[p, chip, core], device_id={"sp": to * 2 + b}, device_id_type=MESH)

    def send(p, i, to):
        for b in range(2):
            @pl.when(to * 2 + b != me)
            def _():
                sending(p, i, b, to).start()

            @pl.when(to * 2 + b == me)
            def _():
                landing(p, chip, core)[...] = part(p, i, b)[...]

    def arrived(p, c):
        for b in range(2):
            @pl.when(c * 2 + b != me)
            def _():
                pltpu.make_async_remote_copy(
                    src_ref=part(p, 0, b), dst_ref=landing(p, c, b), send_sem=send_sem.at[p, 0, b],
                    recv_sem=recv_sem.at[p, c, b], device_id={"sp": c * 2 + b}, device_id_type=MESH).wait_recv()

    x_copy = pltpu.make_async_copy(x_hbm, x_ref, x_sem)
    x_copy.start()
    for t in range(AHEAD):
        load_w(0, t, flipped(chip, SEND[0][t])).start()
    barrier = pltpu.get_barrier_semaphore()
    for n in range(1, 16):
        pl.semaphore_signal(barrier, inc=1, device_id={"sp": lax.rem(me + n, 16)}, device_id_type=MESH)

    values[:, HEAD:, :] = jnp.ones((CHIPS, ONES, PAIR), jnp.bfloat16)
    x_copy.wait()

    def norm(r, _):
        rows = pl.ds(pl.multiple_of(r * 32, 32), 32)
        t = x_ref[rows, :].astype(jnp.float32)
        scale = lax.rsqrt(jnp.mean(t * t, -1, keepdims=True) + 1e-6)
        a_ref[rows, :] = (t * scale * gain_ref[...].astype(jnp.float32)).astype(jnp.bfloat16)

    lax.fori_loop(0, OWN // 32, norm, None)
    pl.semaphore_wait(barrier, 15)

    def turned(t):
        cos, sin = cos_ref[...], sin_ref[...]
        a, b = t[:, : HEAD // 2].astype(jnp.float32), t[:, HEAD // 2 :].astype(jnp.float32)
        return jnp.concatenate([a * cos - b * sin, b * cos + a * sin], -1).astype(jnp.bfloat16)

    for p in range(3):
        def project(i, code, p=p):
            t = p * CHIPS + i
            slot, later = lax.rem(t, AHEAD + 1), lax.rem(t + AHEAD, AHEAD + 1)
            other = flipped(chip, lax.rem(code, 8))
            after = flipped(chip, lax.rem(lax.div(code, 8**AHEAD), 8))

            @pl.when(i < CHIPS - AHEAD)
            def _():
                load_w(p, later, after).start()

            if p < 2:
                @pl.when(i >= CHIPS - AHEAD)
                def _():
                    load_w(p + 1, later, after).start()

            load_w(p, slot, other).wait()
            made = jnp.dot(a_ref[...], w_ref[slot], preferred_element_type=jnp.float32).astype(jnp.bfloat16)
            for b in range(2):
                one = made[:, b * HEAD : (b + 1) * HEAD]
                out_ref[t, b] = one.T if p == 1 else turned(one)
            send(p, i, other)
            return lax.div(code, 8)

        lax.fori_loop(0, CHIPS, project, digits(SEND[p] + (SEND[p + 1][:AHEAD] if p < 2 else [])))

    for t in range(AHEAD):
        load_wo(t, flipped(chip, TAKE[t])).start()
    lax.fori_loop(0, CHIPS, lambda c, _: (arrived(0, c), arrived(1, c), None)[-1], None)

    e = HEAD**-0.5 * LOG2E

    def unit(c, j, first):
        q = queries[c]
        k = keys[j]
        v = values[j]
        strips = [(s, slice(s * 256, (s + 1) * 256)) for s in range(2)]
        scores = [dot(k, q[at, :], 1, 1) for _, at in strips]
        for (s, at), score in zip(strips, scores):
            if first:
                key = lax.broadcasted_iota(jnp.int32, score.shape, 0)
                query = lax.broadcasted_iota(jnp.int32, score.shape, 1) + s * 256
                score = jnp.where(key <= query, score, HIDDEN)
                top = score.max(axis=0, keepdims=True)
            else:
                old = top_s[:, at]
                top = jnp.maximum(old, score.max(axis=0, keepdims=True))
            top_s[:, at] = top
            weights = jnp.exp2((score - top) * e).astype(jnp.bfloat16)
            mix = dot(v, weights, 1, 0)
            mix_s[:, at] = mix if first else mix_s[:, at] * jnp.exp2((old - top) * e) + mix

    def attend(i, code):
        c = flipped(chip, lax.rem(code, 8))
        arrived(2, c)
        unit(c, c, True)
        lax.fori_loop(0, c, lambda j, _: unit(c, j, False), None)
        got = mix_s[:HEAD, :] * (1 / mix_s[HEAD : HEAD + 1, :])
        seen_out[i] = got.astype(jnp.bfloat16).T
        send(3, i, c)
        return lax.div(code, 8)

    lax.fori_loop(0, CHIPS, attend, digits(TAKE))

    TILE = 512

    def spread(i, code):
        slot, later = lax.rem(i, AHEAD + 1), lax.rem(i + AHEAD, AHEAD + 1)
        other = flipped(chip, lax.rem(code, 8))
        after = flipped(chip, lax.rem(lax.div(code, 8**AHEAD), 8))

        @pl.when(i < CHIPS - AHEAD)
        def _():
            load_wo(later, after).start()

        load_wo(slot, other).wait()
        arrived(3, other)
        left = seen_in[:, pl.ds(pl.multiple_of(other * PAIR, PAIR), PAIR)]

        def tile(n, _):
            at = pl.ds(pl.multiple_of(n * TILE, TILE), TILE)
            more = jnp.dot(left, wo_ref[slot, :, at], preferred_element_type=jnp.float32)

            @pl.when(i == 0)
            def _():
                acc_ref[:, at] = more

            @pl.when(i > 0)
            def _():
                acc_ref[:, at] += more

        lax.fori_loop(0, DIM // TILE, tile, None)
        return lax.div(code, 8)

    lax.fori_loop(0, CHIPS, spread, digits(TAKE))

    def finish(n, _):
        at = pl.ds(pl.multiple_of(n * TILE, TILE), TILE)
        x_ref[:, at] = (x_ref[:, at].astype(jnp.float32) + acc_ref[:, at]).astype(jnp.bfloat16)

    lax.fori_loop(0, DIM // TILE, finish, None)
    y_copy = pltpu.make_async_copy(x_ref, y_hbm, y_sem)
    y_copy.start()

    for p in range(4):
        def drain(i, code, p=p):
            to = flipped(chip, lax.rem(code, 8))
            for b in range(2):
                @pl.when(to * 2 + b != me)
                def _():
                    sending(p, i, b, to).wait_send()
            return lax.div(code, 8)

        lax.fori_loop(0, CHIPS, drain, digits((SEND + [TAKE])[p]))
    y_copy.wait()


def solution(mesh):
    def step(x, gain, wq, wk, wv, wo):
        place = lax.axis_index("sp") * OWN + jnp.arange(OWN)
        half = HEAD // 2
        angle = place.astype(jnp.float32)[:, None] * THETA ** (-jnp.arange(half, dtype=jnp.float32) / half)
        vmem, hbm = pl.BlockSpec(memory_space=pltpu.VMEM), pl.BlockSpec(memory_space=pl.ANY)
        bf16, f32 = jnp.bfloat16, jnp.float32
        return pl.pallas_call(
            kernel,
            out_shape=jax.ShapeDtypeStruct((OWN, DIM), bf16),
            in_specs=[hbm, vmem, vmem, vmem, hbm, hbm, hbm, hbm],
            out_specs=hbm,
            scratch_shapes=[
                pltpu.VMEM((OWN, DIM), bf16),
                pltpu.VMEM((OWN, DIM), bf16),
                pltpu.VMEM((AHEAD + 1, DIM, PAIR), bf16),
                pltpu.VMEM((AHEAD + 1, PAIR, DIM), bf16),
                pltpu.VMEM((3 * CHIPS, 2, OWN, HEAD), bf16),
                pltpu.VMEM((CHIPS, PAIR, HEAD), bf16),
                pltpu.VMEM((CHIPS, HEAD + ONES, PAIR), bf16),
                pltpu.VMEM((CHIPS, PAIR, HEAD), bf16),
                pltpu.VMEM((CHIPS, PAIR, HEAD), bf16),
                pltpu.VMEM((OWN, DIM), bf16),
                pltpu.VMEM((1, PAIR), f32),
                pltpu.VMEM((HEAD + ONES, PAIR), f32),
                pltpu.VMEM((OWN, DIM), f32),
                pltpu.SemaphoreType.DMA,
                pltpu.SemaphoreType.DMA((AHEAD + 1,)),
                pltpu.SemaphoreType.DMA((AHEAD + 1,)),
                pltpu.SemaphoreType.DMA,
                pltpu.SemaphoreType.DMA((4, CHIPS, 2)),
                pltpu.SemaphoreType.DMA((4, CHIPS, 2)),
            ],
            compiler_params=pltpu.CompilerParams(collective_id=0, has_side_effects=True, vmem_limit_bytes=63 * 2**20),
            cost_estimate=pl.CostEstimate(flops=2 * OWN * DIM * DIM * 4 + 2 * 2 * 36 * PAIR * PAIR * HEAD, transcendentals=36 * PAIR * PAIR,
                                          bytes_accessed=4 * DIM * DIM * 2),
        )(x, gain.reshape(1, DIM), jnp.cos(angle), jnp.sin(angle), wq, wk, wv, wo)

    tokens, whole = P(("dp", "sp"), None), P(None, None)
    return jax.shard_map(
        step,
        mesh=mesh,
        in_specs=(tokens, P(None), whole, whole, whole, whole),
        out_specs=tokens,
        check_vma=False,
    )
```

```python
import math

import jax
import jax.numpy as jnp
from jax import lax
from jax.experimental import pallas as pl
from jax.experimental.pallas import tpu as pltpu
from jax.sharding import PartitionSpec as P

HEAD = 256
THETA = 10000
LOG2E = 1.4426950408889634
HIDDEN = -2e30
MESH = pl.DeviceIdType.MESH
OWN = 256
PAIR = 2 * HEAD
CHIPS = 8
DIM = 4096
ONES = 16
AHEAD = 2
TILE = PAIR
LAG = 4

LINKS = [6, 1, 5, 2, 3, 4, 7]
SEND = [LINKS + [0], LINKS + [0], [0] + LINKS]
TAKE = [0] + LINKS


def digits(values):
    return sum(v * 8**i for i, v in enumerate(values))


def flipped(n, mask):
    out = n
    for b in range(3):
        bit = lax.rem(lax.div(n, 2**b), 2)
        flip = lax.rem(lax.div(mask, 2**b), 2)
        out = out + flip * (1 - 2 * bit) * 2**b
    return out


def dot(a, b, ca, cb):
    return lax.dot_general(a, b, (((ca,), (cb,)), ((), ())), preferred_element_type=jnp.float32)


def kernel(x_hbm, gain_hbm, wq_hbm, wk_hbm, wv_hbm, wo_hbm, y_ref,
           x_ref, gain_ref, a_ref, cos_ref, sin_ref, w_ref, out_ref, keys, values, queries, seen_out, seen_in, top_s, mix_s, acc_ref,
           x_sem, gain_sem, w_sem, send_sem, recv_sem):
    me = lax.axis_index("sp")
    chip, core = lax.div(me, 2), lax.rem(me, 2)
    wide = [wk_hbm, wv_hbm, wq_hbm]

    def load_w(p, slot, other):
        return pltpu.make_async_copy(wide[p].at[:, pl.ds(pl.multiple_of(other * PAIR, PAIR), PAIR)], w_ref.at[slot], w_sem.at[slot])

    def load_wo(slot, other):
        for n in range(DIM // TILE):
            pltpu.make_async_copy(wo_hbm.at[pl.ds(pl.multiple_of(other * PAIR, PAIR), PAIR), pl.ds(n * TILE, TILE)],
                                  w_ref.at[slot, pl.ds(n * PAIR, PAIR), :], w_sem.at[slot]).start()

    def landing(p, c, b):
        at = pl.ds(pl.multiple_of(b * OWN, OWN), OWN)
        if p == 0:
            return keys.at[c, at, :]
        if p == 1:
            return values.at[c, pl.ds(0, HEAD), at]
        if p == 2:
            return queries.at[c, at, :]
        return seen_in.at[:, pl.ds(pl.multiple_of(c * PAIR + b * HEAD, HEAD), HEAD)]

    def part(p, i, b):
        if p < 3:
            return out_ref.at[p * CHIPS + i, b]
        return seen_out.at[i, pl.ds(b * OWN, OWN), :]

    def sending(p, i, b, to):
        return pltpu.make_async_remote_copy(
            src_ref=part(p, i, b), dst_ref=landing(p, chip, core), send_sem=send_sem.at[p, i, b],
            recv_sem=recv_sem.at[p, chip, core], device_id={"sp": to * 2 + b}, device_id_type=MESH)

    def send(p, i, to):
        for b in range(2):
            @pl.when(to * 2 + b != me)
            def _():
                sending(p, i, b, to).start()

            @pl.when(to * 2 + b == me)
            def _():
                landing(p, chip, core)[...] = part(p, i, b)[...]

    def arrived(p, c):
        for b in range(2):
            @pl.when(c * 2 + b != me)
            def _():
                pltpu.make_async_remote_copy(
                    src_ref=part(p, 0, b), dst_ref=landing(p, c, b), send_sem=send_sem.at[p, 0, b],
                    recv_sem=recv_sem.at[p, c, b], device_id={"sp": c * 2 + b}, device_id_type=MESH).wait_recv()

    x_copy = pltpu.make_async_copy(x_hbm, x_ref, x_sem)
    x_copy.start()
    gain_copy = pltpu.make_async_copy(gain_hbm, gain_ref, gain_sem)
    gain_copy.start()
    for t in range(AHEAD):
        load_w(0, t, flipped(chip, SEND[0][t])).start()
    barrier = pltpu.get_barrier_semaphore()
    for n in range(1, 16):
        pl.semaphore_signal(barrier, inc=1, device_id={"sp": lax.rem(me + n, 16)}, device_id_type=MESH)

    half = HEAD // 2
    place = lax.broadcasted_iota(jnp.int32, (OWN, half), 0) + me * OWN
    power = lax.broadcasted_iota(jnp.int32, (1, half), 1).astype(jnp.float32) * (-math.log2(THETA) / half)
    angle = place.astype(jnp.float32) * jnp.exp2(power)
    cos_ref[...] = jnp.cos(angle)
    sin_ref[...] = jnp.sin(angle)
    values[:, HEAD:, :] = jnp.ones((CHIPS, ONES, PAIR), jnp.bfloat16)
    x_copy.wait()
    gain_copy.wait()

    def norm(r, _):
        rows = pl.ds(pl.multiple_of(r * 32, 32), 32)
        t = x_ref[rows, :].astype(jnp.float32)
        scale = lax.rsqrt(jnp.mean(t * t, -1, keepdims=True) + 1e-6)
        acc_ref[rows, :] = t
        a_ref[rows, :] = (t * scale * gain_ref[...].reshape(1, DIM).astype(jnp.float32)).astype(jnp.bfloat16)

    lax.fori_loop(0, OWN // 32, norm, None)
    pl.semaphore_wait(barrier, 15)

    def turned(t):
        cos, sin = cos_ref[...], sin_ref[...]
        a, b = t[:, : HEAD // 2].astype(jnp.float32), t[:, HEAD // 2 :].astype(jnp.float32)
        return jnp.concatenate([a * cos - b * sin, b * cos + a * sin], -1).astype(jnp.bfloat16)

    for p in range(3):
        def project(i, code, p=p):
            t = p * CHIPS + i
            slot, later = lax.rem(t, AHEAD + 1), lax.rem(t + AHEAD, AHEAD + 1)
            other = flipped(chip, lax.rem(code, 8))
            after = flipped(chip, lax.rem(lax.div(code, 8**AHEAD), 8))

            @pl.when(i < CHIPS - AHEAD)
            def _():
                load_w(p, later, after).start()

            @pl.when(i >= CHIPS - AHEAD)
            def _():
                if p < 2:
                    load_w(p + 1, later, after).start()
                else:
                    load_wo(later, after)

            load_w(p, slot, other).wait()
            made = jnp.dot(a_ref[...], w_ref[slot], preferred_element_type=jnp.float32).astype(jnp.bfloat16)
            for b in range(2):
                one = made[:, b * HEAD : (b + 1) * HEAD]
                out_ref[t, b] = one.T if p == 1 else turned(one)
            send(p, i, other)
            return lax.div(code, 8)

        lax.fori_loop(0, CHIPS, project, digits(SEND[p] + (SEND + [TAKE])[p + 1][:AHEAD]))

    lax.fori_loop(0, CHIPS, lambda c, _: (arrived(0, c), arrived(1, c), None)[-1], None)

    e = HEAD**-0.5 * LOG2E

    def unit(c, j, first):
        q = queries[c]
        k = keys[j]
        v = values[j]
        strips = [(s, slice(s * 256, (s + 1) * 256)) for s in range(2)]
        scores = [dot(k, q[at, :], 1, 1) for _, at in strips]
        for (s, at), score in zip(strips, scores):
            if first:
                key = lax.broadcasted_iota(jnp.int32, score.shape, 0)
                query = lax.broadcasted_iota(jnp.int32, score.shape, 1) + s * 256
                score = jnp.where(key <= query, score, HIDDEN)
                top = score.max(axis=0, keepdims=True)
            else:
                old = top_s[:, at]
                top = jnp.maximum(old, score.max(axis=0, keepdims=True))
            top_s[:, at] = top
            weights = jnp.exp2((score - top) * e).astype(jnp.bfloat16)
            mix = dot(v, weights, 1, 0)
            mix_s[:, at] = mix if first else mix_s[:, at] * jnp.exp2((old - top) * e) + mix

    def attend(i, code):
        c = flipped(chip, lax.rem(code, 8))
        arrived(2, c)
        unit(c, c, True)
        lax.fori_loop(0, c, lambda j, _: unit(c, j, False), None)
        got = mix_s[:HEAD, :] * (1 / mix_s[HEAD : HEAD + 1, :])
        seen_out[i] = got.astype(jnp.bfloat16).T
        send(3, i, c)
        return lax.div(code, 8)

    def spread(i, code):
        t = 3 * CHIPS + i
        slot, later = lax.rem(t, AHEAD + 1), lax.rem(t + AHEAD, AHEAD + 1)
        other = flipped(chip, lax.rem(code, 8))
        after = flipped(chip, lax.rem(lax.div(code, 8**AHEAD), 8))

        @pl.when(i < CHIPS - AHEAD)
        def _():
            load_wo(later, after)

        load_w(0, slot, other).wait()
        arrived(3, other)
        left = seen_in[:, pl.ds(pl.multiple_of(other * PAIR, PAIR), PAIR)]
        for n in range(DIM // TILE):
            at = slice(n * TILE, (n + 1) * TILE)
            acc_ref[:, at] += jnp.dot(left, w_ref[slot, n * PAIR : (n + 1) * PAIR, :], preferred_element_type=jnp.float32)
        return lax.div(code, 8)

    def both(i, codes):
        return attend(i, codes[0]), spread(i - LAG, codes[1])

    code = lax.fori_loop(0, LAG, attend, digits(TAKE))
    code = lax.fori_loop(LAG, CHIPS, both, (code, digits(TAKE)))[1]
    lax.fori_loop(CHIPS - LAG, CHIPS, spread, code)
    y_ref[...] = acc_ref[...].astype(jnp.bfloat16)

    for p in range(4):
        def drain(i, code, p=p):
            to = flipped(chip, lax.rem(code, 8))
            for b in range(2):
                @pl.when(to * 2 + b != me)
                def _():
                    sending(p, i, b, to).wait_send()
            return lax.div(code, 8)

        lax.fori_loop(0, CHIPS, drain, digits((SEND + [TAKE])[p]))


def solution(mesh):
    def step(x, gain, wq, wk, wv, wo):
        vmem, hbm = pl.BlockSpec(memory_space=pltpu.VMEM), pl.BlockSpec(memory_space=pltpu.HBM)
        bf16, f32 = jnp.bfloat16, jnp.float32
        return pl.pallas_call(
            kernel,
            out_shape=jax.ShapeDtypeStruct((OWN, DIM), bf16),
            in_specs=[hbm] * 6,
            out_specs=vmem,
            scratch_shapes=[
                pltpu.VMEM((OWN, DIM), bf16),
                pltpu.VMEM((DIM,), bf16),
                pltpu.VMEM((OWN, DIM), bf16),
                pltpu.VMEM((OWN, HEAD // 2), f32),
                pltpu.VMEM((OWN, HEAD // 2), f32),
                pltpu.VMEM((AHEAD + 1, DIM, PAIR), bf16),
                pltpu.VMEM((3 * CHIPS, 2, OWN, HEAD), bf16),
                pltpu.VMEM((CHIPS, PAIR, HEAD), bf16),
                pltpu.VMEM((CHIPS, HEAD + ONES, PAIR), bf16),
                pltpu.VMEM((CHIPS, PAIR, HEAD), bf16),
                pltpu.VMEM((CHIPS, PAIR, HEAD), bf16),
                pltpu.VMEM((OWN, DIM), bf16),
                pltpu.VMEM((1, PAIR), f32),
                pltpu.VMEM((HEAD + ONES, PAIR), f32),
                pltpu.VMEM((OWN, DIM), f32),
                pltpu.SemaphoreType.DMA,
                pltpu.SemaphoreType.DMA,
                pltpu.SemaphoreType.DMA((AHEAD + 1,)),
                pltpu.SemaphoreType.DMA((4, CHIPS, 2)),
                pltpu.SemaphoreType.DMA((4, CHIPS, 2)),
            ],
            compiler_params=pltpu.CompilerParams(collective_id=0, has_side_effects=True, vmem_limit_bytes=44 * 2**20),
            cost_estimate=pl.CostEstimate(flops=2 * OWN * DIM * DIM * 4 + 2 * 2 * 36 * PAIR * PAIR * HEAD, transcendentals=36 * PAIR * PAIR,
                                          bytes_accessed=4 * DIM * DIM * 2),
        )(*(pltpu.with_memory_space_constraint(t, pltpu.HBM) for t in (x, gain)), wq, wk, wv, wo)

    tokens, whole = P(("dp", "sp"), None), P(None, None)
    return jax.shard_map(
        step,
        mesh=mesh,
        in_specs=(tokens, P(None), whole, whole, whole, whole),
        out_specs=tokens,
        check_vma=False,
    )
```

```python
import math

import jax
import jax.numpy as jnp
from jax import lax
from jax.experimental import pallas as pl
from jax.experimental.pallas import tpu as pltpu
from jax.sharding import PartitionSpec as P

HEAD = 256
THETA = 10000
LOG2E = 1.4426950408889634
HIDDEN = -2e30
MESH = pl.DeviceIdType.MESH
OWN = 256
PAIR = 2 * HEAD
CHIPS = 8
DIM = 4096
ONES = 16
AHEAD = 2
TILE = PAIR
LAG = 4

LINKS = [7, 6, 1, 5, 2, 3, 4]
SEND = [LINKS + [0], LINKS + [0], [0] + LINKS]
TAKE = [0] + LINKS


def digits(values):
    return sum(v * 8**i for i, v in enumerate(values))


def flipped(n, mask):
    out = n
    for b in range(3):
        bit = lax.rem(lax.div(n, 2**b), 2)
        flip = lax.rem(lax.div(mask, 2**b), 2)
        out = out + flip * (1 - 2 * bit) * 2**b
    return out


def dot(a, b, ca, cb):
    return lax.dot_general(a, b, (((ca,), (cb,)), ((), ())), preferred_element_type=jnp.float32)


def kernel(x_hbm, gain_hbm, wq_hbm, wk_hbm, wv_hbm, wo_hbm, y_ref,
           x_ref, gain_ref, a_ref, cos_ref, sin_ref, w_ref, out_ref, keys, values, queries, seen_out, seen_in, top_s, mix_s, acc_ref,
           x_sem, gain_sem, w_sem, send_sem, recv_sem):
    me = lax.axis_index("sp")
    chip, core = lax.div(me, 2), lax.rem(me, 2)
    wide = [wk_hbm, wv_hbm, wq_hbm]

    def load_w(p, slot, other):
        return pltpu.make_async_copy(wide[p].at[:, pl.ds(pl.multiple_of(other * PAIR, PAIR), PAIR)], w_ref.at[slot], w_sem.at[slot])

    def load_wo(slot, other):
        for n in range(DIM // TILE):
            pltpu.make_async_copy(wo_hbm.at[pl.ds(pl.multiple_of(other * PAIR, PAIR), PAIR), pl.ds(n * TILE, TILE)],
                                  w_ref.at[slot, pl.ds(n * PAIR, PAIR), :], w_sem.at[slot]).start()

    def landing(p, c, b):
        at = pl.ds(pl.multiple_of(b * OWN, OWN), OWN)
        if p == 0:
            return keys.at[c, at, :]
        if p == 1:
            return values.at[c, pl.ds(0, HEAD), at]
        if p == 2:
            return queries.at[c, at, :]
        return seen_in.at[:, pl.ds(pl.multiple_of(c * PAIR + b * HEAD, HEAD), HEAD)]

    def part(p, i, b):
        if p < 3:
            return out_ref.at[p * CHIPS + i, b]
        return seen_out.at[i, pl.ds(b * OWN, OWN), :]

    def sending(p, i, b, to):
        return pltpu.make_async_remote_copy(
            src_ref=part(p, i, b), dst_ref=landing(p, chip, core), send_sem=send_sem.at[p, i, b],
            recv_sem=recv_sem.at[p, chip, core], device_id={"sp": to * 2 + b}, device_id_type=MESH)

    def send(p, i, to):
        for b in range(2):
            @pl.when(to * 2 + b != me)
            def _():
                sending(p, i, b, to).start()

            @pl.when(to * 2 + b == me)
            def _():
                landing(p, chip, core)[...] = part(p, i, b)[...]

    def arrived(p, c):
        for b in range(2):
            @pl.when(c * 2 + b != me)
            def _():
                pltpu.make_async_remote_copy(
                    src_ref=part(p, 0, b), dst_ref=landing(p, c, b), send_sem=send_sem.at[p, 0, b],
                    recv_sem=recv_sem.at[p, c, b], device_id={"sp": c * 2 + b}, device_id_type=MESH).wait_recv()

    x_copies = [pltpu.make_async_copy(x_hbm.at[pl.ds(n * 64, 64)], x_ref.at[pl.ds(n * 64, 64)], x_sem.at[n]) for n in range(4)]
    for x_copy in x_copies:
        x_copy.start()
    gain_copy = pltpu.make_async_copy(gain_hbm, gain_ref, gain_sem)
    gain_copy.start()
    load_w(0, 0, flipped(chip, SEND[0][0])).start()
    barrier = pltpu.get_barrier_semaphore()
    for n in range(1, 16):
        pl.semaphore_signal(barrier, inc=1, device_id={"sp": lax.rem(me + n, 16)}, device_id_type=MESH)

    half = HEAD // 2
    place = lax.broadcasted_iota(jnp.int32, (OWN, half), 0) + me * OWN
    power = lax.broadcasted_iota(jnp.int32, (1, half), 1).astype(jnp.float32) * (-math.log2(THETA) / half)
    angle = place.astype(jnp.float32) * jnp.exp2(power)
    cos_ref[...] = jnp.cos(angle)
    sin_ref[...] = jnp.sin(angle)
    values[:, HEAD:, :] = jnp.ones((CHIPS, ONES, PAIR), jnp.bfloat16)
    gain_copy.wait()

    def norm(r, _):
        rows = pl.ds(pl.multiple_of(r * 32, 32), 32)
        t = x_ref[rows, :].astype(jnp.float32)
        scale = lax.rsqrt(jnp.mean(t * t, -1, keepdims=True) + 1e-6)
        acc_ref[rows, :] = t
        a_ref[rows, :] = (t * scale * gain_ref[...].reshape(1, DIM).astype(jnp.float32)).astype(jnp.bfloat16)

    for n in range(4):
        x_copies[n].wait()
        lax.fori_loop(n * 2, n * 2 + 2, norm, None)
    load_w(0, 1, flipped(chip, SEND[0][1])).start()
    pl.semaphore_wait(barrier, 15)

    def turned(t):
        cos, sin = cos_ref[...], sin_ref[...]
        a, b = t[:, : HEAD // 2].astype(jnp.float32), t[:, HEAD // 2 :].astype(jnp.float32)
        return jnp.concatenate([a * cos - b * sin, b * cos + a * sin], -1).astype(jnp.bfloat16)

    for p in range(3):
        def project(i, code, p=p):
            t = p * CHIPS + i
            slot, later = lax.rem(t, AHEAD + 1), lax.rem(t + AHEAD, AHEAD + 1)
            other = flipped(chip, lax.rem(code, 8))
            after = flipped(chip, lax.rem(lax.div(code, 8**AHEAD), 8))

            @pl.when(i < CHIPS - AHEAD)
            def _():
                load_w(p, later, after).start()

            @pl.when(i >= CHIPS - AHEAD)
            def _():
                if p < 2:
                    load_w(p + 1, later, after).start()
                else:
                    load_wo(later, after)

            load_w(p, slot, other).wait()
            made = jnp.dot(a_ref[...], w_ref[slot], preferred_element_type=jnp.float32).astype(jnp.bfloat16)
            for b in range(2):
                one = made[:, b * HEAD : (b + 1) * HEAD]
                out_ref[t, b] = one.T if p == 1 else turned(one)
            send(p, i, other)
            return lax.div(code, 8)

        lax.fori_loop(0, CHIPS, project, digits(SEND[p] + (SEND + [TAKE])[p + 1][:AHEAD]))

    lax.fori_loop(0, CHIPS, lambda c, _: (arrived(0, c), arrived(1, c), None)[-1], None)

    e = HEAD**-0.5 * LOG2E

    def unit(c, j, first):
        q = queries[c]
        k = keys[j]
        v = values[j]
        strips = [(s, slice(s * 256, (s + 1) * 256)) for s in range(2)]
        scores = [dot(k, q[at, :], 1, 1) for _, at in strips]
        for (s, at), score in zip(strips, scores):
            if first:
                key = lax.broadcasted_iota(jnp.int32, score.shape, 0)
                query = lax.broadcasted_iota(jnp.int32, score.shape, 1) + s * 256
                score = jnp.where(key <= query, score, HIDDEN)
                top = score.max(axis=0, keepdims=True)
            else:
                old = top_s[:, at]
                top = jnp.maximum(old, score.max(axis=0, keepdims=True))
            top_s[:, at] = top
            weights = jnp.exp2((score - top) * e).astype(jnp.bfloat16)
            mix = dot(v, weights, 1, 0)
            mix_s[:, at] = mix if first else mix_s[:, at] * jnp.exp2((old - top) * e) + mix

    def attend(i, code):
        c = flipped(chip, lax.rem(code, 8))
        arrived(2, c)
        unit(c, c, True)
        lax.fori_loop(0, c, lambda j, _: unit(c, j, False), None)
        got = mix_s[:HEAD, :] * (1 / mix_s[HEAD : HEAD + 1, :])
        seen_out[i] = got.astype(jnp.bfloat16).T
        send(3, i, c)
        return lax.div(code, 8)

    def spread(i, code, last=False):
        t = 3 * CHIPS + i
        slot, later = lax.rem(t, AHEAD + 1), lax.rem(t + AHEAD, AHEAD + 1)
        other = flipped(chip, lax.rem(code, 8))
        after = flipped(chip, lax.rem(lax.div(code, 8**AHEAD), 8))

        @pl.when(i < CHIPS - AHEAD)
        def _():
            load_wo(later, after)

        load_w(0, slot, other).wait()
        arrived(3, other)
        left = seen_in[:, pl.ds(pl.multiple_of(other * PAIR, PAIR), PAIR)]
        for n in range(DIM // TILE):
            at = slice(n * TILE, (n + 1) * TILE)
            total = acc_ref[:, at] + jnp.dot(left, w_ref[slot, n * PAIR : (n + 1) * PAIR, :], preferred_element_type=jnp.float32)
            if last:
                y_ref[:, at] = total.astype(jnp.bfloat16)
            else:
                acc_ref[:, at] = total
        return lax.div(code, 8)

    def both(i, codes):
        return attend(i, codes[0]), spread(i - LAG, codes[1])

    code = lax.fori_loop(0, LAG, attend, digits(TAKE))
    code = lax.fori_loop(LAG, CHIPS, both, (code, digits(TAKE)))[1]
    code = lax.fori_loop(CHIPS - LAG, CHIPS - 1, spread, code)
    spread(CHIPS - 1, code, True)

    for p in range(4):
        def drain(i, code, p=p):
            to = flipped(chip, lax.rem(code, 8))
            for b in range(2):
                @pl.when(to * 2 + b != me)
                def _():
                    sending(p, i, b, to).wait_send()
            return lax.div(code, 8)

        lax.fori_loop(0, CHIPS, drain, digits((SEND + [TAKE])[p]))


def solution(mesh):
    def step(x, gain, wq, wk, wv, wo):
        vmem, hbm = pl.BlockSpec(memory_space=pltpu.VMEM), pl.BlockSpec(memory_space=pltpu.HBM)
        bf16, f32 = jnp.bfloat16, jnp.float32
        return pl.pallas_call(
            kernel,
            out_shape=jax.ShapeDtypeStruct((OWN, DIM), bf16),
            in_specs=[hbm] * 6,
            out_specs=vmem,
            scratch_shapes=[
                pltpu.VMEM((OWN, DIM), bf16),
                pltpu.VMEM((DIM,), bf16),
                pltpu.VMEM((OWN, DIM), bf16),
                pltpu.VMEM((OWN, HEAD // 2), f32),
                pltpu.VMEM((OWN, HEAD // 2), f32),
                pltpu.VMEM((AHEAD + 1, DIM, PAIR), bf16),
                pltpu.VMEM((3 * CHIPS, 2, OWN, HEAD), bf16),
                pltpu.VMEM((CHIPS, PAIR, HEAD), bf16),
                pltpu.VMEM((CHIPS, HEAD + ONES, PAIR), bf16),
                pltpu.VMEM((CHIPS, PAIR, HEAD), bf16),
                pltpu.VMEM((CHIPS, PAIR, HEAD), bf16),
                pltpu.VMEM((OWN, DIM), bf16),
                pltpu.VMEM((1, PAIR), f32),
                pltpu.VMEM((HEAD + ONES, PAIR), f32),
                pltpu.VMEM((OWN, DIM), f32),
                pltpu.SemaphoreType.DMA((4,)),
                pltpu.SemaphoreType.DMA,
                pltpu.SemaphoreType.DMA((AHEAD + 1,)),
                pltpu.SemaphoreType.DMA((4, CHIPS, 2)),
                pltpu.SemaphoreType.DMA((4, CHIPS, 2)),
            ],
            compiler_params=pltpu.CompilerParams(collective_id=0, has_side_effects=True, vmem_limit_bytes=44 * 2**20),
            cost_estimate=pl.CostEstimate(flops=2 * OWN * DIM * DIM * 4 + 2 * 2 * 36 * PAIR * PAIR * HEAD, transcendentals=36 * PAIR * PAIR,
                                          bytes_accessed=4 * DIM * DIM * 2),
        )(*(pltpu.with_memory_space_constraint(t, pltpu.HBM) for t in (x, gain)), wq, wk, wv, wo)

    tokens, whole = P(("dp", "sp"), None), P(None, None)
    return jax.shard_map(
        step,
        mesh=mesh,
        in_specs=(tokens, P(None), whole, whole, whole, whole),
        out_specs=tokens,
        check_vma=False,
    )
```

```python
import functools
import math

import jax
import jax.numpy as jnp
from jax import lax
from jax.experimental import pallas as pl
from jax.experimental.pallas import tpu as pltpu
from jax.sharding import PartitionSpec as P

HEAD = 256
THETA = 10000
LOG2E = 1.4426950408889634
HIDDEN = -2e30
MESH = pl.DeviceIdType.MESH
OWN = 256
PAIR = 2 * HEAD
CHIPS = 8
DIM = 4096
ONES = 16
AHEAD = 2
TILE = PAIR
LAG = 4

LINKS = [7, 6, 1, 5, 2, 3, 4]
SEND = [LINKS + [0], LINKS + [0], [0] + LINKS]
TAKE = [0] + LINKS


def digits(values):
    return sum(v * 8**i for i, v in enumerate(values))


def flipped(n, mask):
    out = n
    for b in range(3):
        bit = lax.rem(lax.div(n, 2**b), 2)
        flip = lax.rem(lax.div(mask, 2**b), 2)
        out = out + flip * (1 - 2 * bit) * 2**b
    return out


def dot(a, b, ca, cb):
    return lax.dot_general(a, b, (((ca,), (cb,)), ((), ())), preferred_element_type=jnp.float32)


def kernel(x_hbm, gain_hbm, wq_hbm, wk_hbm, wv_hbm, wo_hbm, y_ref,
           x_ref, gain_ref, a_ref, cos_ref, sin_ref, w_ref, out_ref, keys, values, queries, seen_out, seen_in, top_s, mix_s, acc_ref,
           x_sem, gain_sem, w_sem, send_sem, recv_sem):
    me = lax.axis_index("sp")
    chip, core = lax.div(me, 2), lax.rem(me, 2)
    wide = [wk_hbm, wv_hbm, wq_hbm]

    def load_w(p, slot, other):
        return pltpu.make_async_copy(wide[p].at[:, pl.ds(pl.multiple_of(other * PAIR, PAIR), PAIR)], w_ref.at[slot], w_sem.at[slot])

    def load_wo(slot, other):
        for n in range(DIM // TILE):
            pltpu.make_async_copy(wo_hbm.at[pl.ds(pl.multiple_of(other * PAIR, PAIR), PAIR), pl.ds(n * TILE, TILE)],
                                  w_ref.at[slot, pl.ds(n * PAIR, PAIR), :], w_sem.at[slot]).start()

    def landing(p, c, b):
        at = pl.ds(pl.multiple_of(b * OWN, OWN), OWN)
        if p == 0:
            return keys.at[c, at, :]
        if p == 1:
            return values.at[c, pl.ds(0, HEAD), at]
        if p == 2:
            return queries.at[c, at, :]
        return seen_in.at[:, pl.ds(pl.multiple_of(c * PAIR + b * HEAD, HEAD), HEAD)]

    def part(p, i, b):
        if p < 3:
            return out_ref.at[p * CHIPS + i, b]
        return seen_out.at[i, pl.ds(b * OWN, OWN), :]

    def sending(p, i, b, to):
        return pltpu.make_async_remote_copy(
            src_ref=part(p, i, b), dst_ref=landing(p, chip, core), send_sem=send_sem.at[p, i, b],
            recv_sem=recv_sem.at[p, chip, core], device_id={"sp": to * 2 + b}, device_id_type=MESH)

    def send(p, i, to):
        for b in range(2):
            @pl.when(to * 2 + b != me)
            def _():
                sending(p, i, b, to).start()

            @pl.when(to * 2 + b == me)
            def _():
                landing(p, chip, core)[...] = part(p, i, b)[...]

    def arrived(p, c):
        for b in range(2):
            @pl.when(c * 2 + b != me)
            def _():
                pltpu.make_async_remote_copy(
                    src_ref=part(p, 0, b), dst_ref=landing(p, c, b), send_sem=send_sem.at[p, 0, b],
                    recv_sem=recv_sem.at[p, c, b], device_id={"sp": c * 2 + b}, device_id_type=MESH).wait_recv()

    x_copies = [pltpu.make_async_copy(x_hbm.at[pl.ds(n * 64, 64)], x_ref.at[pl.ds(n * 64, 64)], x_sem.at[n]) for n in range(4)]
    for x_copy in x_copies:
        x_copy.start()
    gain_copy = pltpu.make_async_copy(gain_hbm, gain_ref, gain_sem)
    gain_copy.start()
    load_w(0, 0, flipped(chip, SEND[0][0])).start()
    barrier = pltpu.get_barrier_semaphore()
    for n in range(1, 16):
        pl.semaphore_signal(barrier, inc=1, device_id={"sp": lax.rem(me + n, 16)}, device_id_type=MESH)

    half = HEAD // 2
    place = lax.broadcasted_iota(jnp.int32, (OWN, half), 0) + me * OWN
    power = lax.broadcasted_iota(jnp.int32, (1, half), 1).astype(jnp.float32) * (-math.log2(THETA) / half)
    angle = place.astype(jnp.float32) * jnp.exp2(power)
    cos_ref[...] = jnp.cos(angle)
    sin_ref[...] = jnp.sin(angle)
    values[:, HEAD:, :] = jnp.ones((CHIPS, ONES, PAIR), jnp.bfloat16)
    gain_copy.wait()

    def norm(r, _):
        rows = pl.ds(pl.multiple_of(r * 32, 32), 32)
        t = x_ref[rows, :].astype(jnp.float32)
        scale = lax.rsqrt(jnp.mean(t * t, -1, keepdims=True) + 1e-6)
        acc_ref[rows, :] = t
        a_ref[rows, :] = (t * scale * gain_ref[...].reshape(1, DIM).astype(jnp.float32)).astype(jnp.bfloat16)

    for n in range(4):
        x_copies[n].wait()
        lax.fori_loop(n * 2, n * 2 + 2, norm, None)
    load_w(0, 1, flipped(chip, SEND[0][1])).start()
    pl.semaphore_wait(barrier, 15)

    def turned(t):
        cos, sin = cos_ref[...], sin_ref[...]
        a, b = t[:, : HEAD // 2].astype(jnp.float32), t[:, HEAD // 2 :].astype(jnp.float32)
        return jnp.concatenate([a * cos - b * sin, b * cos + a * sin], -1).astype(jnp.bfloat16)

    for p in range(3):
        def project(i, code, p=p):
            t = p * CHIPS + i
            slot, later = lax.rem(t, AHEAD + 1), lax.rem(t + AHEAD, AHEAD + 1)
            other = flipped(chip, lax.rem(code, 8))
            after = flipped(chip, lax.rem(lax.div(code, 8**AHEAD), 8))

            @pl.when(i < CHIPS - AHEAD)
            def _():
                load_w(p, later, after).start()

            @pl.when(i >= CHIPS - AHEAD)
            def _():
                if p < 2:
                    load_w(p + 1, later, after).start()
                else:
                    load_wo(later, after)

            load_w(p, slot, other).wait()
            made = jnp.dot(a_ref[...], w_ref[slot], preferred_element_type=jnp.float32).astype(jnp.bfloat16)
            for b in range(2):
                one = made[:, b * HEAD : (b + 1) * HEAD]
                out_ref[t, b] = one.T if p == 1 else turned(one)
            send(p, i, other)
            return lax.div(code, 8)

        lax.fori_loop(0, CHIPS, project, digits(SEND[p] + (SEND + [TAKE])[p + 1][:AHEAD]))

    lax.fori_loop(0, CHIPS, lambda c, _: (arrived(0, c), arrived(1, c), None)[-1], None)

    e = HEAD**-0.5 * LOG2E

    def unit(c, blocks, first=False):
        q = queries[c]
        strips = [(s, slice(s * 256, (s + 1) * 256)) for s in range(2)]
        scores = [[dot(keys[j], q[at, :], 1, 1) for j in blocks] for _, at in strips]
        for (s, at), score in zip(strips, scores):
            if first:
                key = lax.broadcasted_iota(jnp.int32, score[0].shape, 0)
                query = lax.broadcasted_iota(jnp.int32, score[0].shape, 1) + s * 256
                score = [jnp.where(key <= query, score[0], HIDDEN)]
            top = functools.reduce(jnp.maximum, [t.max(axis=0, keepdims=True) for t in score])
            if not first:
                old = top_s[:, at]
                top = jnp.maximum(old, top)
            top_s[:, at] = top
            weights = [jnp.exp2((t - top) * e).astype(jnp.bfloat16) for t in score]
            mix = sum(dot(values[j], w, 1, 0) for j, w in zip(blocks, weights))
            mix_s[:, at] = mix if first else mix_s[:, at] * jnp.exp2((old - top) * e) + mix

    def attend(i, code):
        c = flipped(chip, lax.rem(code, 8))
        arrived(2, c)
        unit(c, (c,), True)
        lax.fori_loop(0, lax.div(c, 2), lambda j, _: unit(c, (2 * j, 2 * j + 1)), None)

        @pl.when(lax.rem(c, 2) == 1)
        def _():
            unit(c, (c - 1,))

        got = mix_s[:HEAD, :] * (1 / mix_s[HEAD : HEAD + 1, :])
        seen_out[i] = got.astype(jnp.bfloat16).T
        send(3, i, c)
        return lax.div(code, 8)

    def spread(i, code, last=False):
        t = 3 * CHIPS + i
        slot, later = lax.rem(t, AHEAD + 1), lax.rem(t + AHEAD, AHEAD + 1)
        other = flipped(chip, lax.rem(code, 8))
        after = flipped(chip, lax.rem(lax.div(code, 8**AHEAD), 8))

        @pl.when(i < CHIPS - AHEAD)
        def _():
            load_wo(later, after)

        load_w(0, slot, other).wait()
        arrived(3, other)
        left = seen_in[:, pl.ds(pl.multiple_of(other * PAIR, PAIR), PAIR)]
        for n in range(DIM // TILE):
            at = slice(n * TILE, (n + 1) * TILE)
            total = acc_ref[:, at] + jnp.dot(left, w_ref[slot, n * PAIR : (n + 1) * PAIR, :], preferred_element_type=jnp.float32)
            if last:
                y_ref[:, at] = total.astype(jnp.bfloat16)
            else:
                acc_ref[:, at] = total
        return lax.div(code, 8)

    def both(i, codes):
        return attend(i, codes[0]), spread(i - LAG, codes[1])

    code = lax.fori_loop(0, LAG, attend, digits(TAKE))
    code = lax.fori_loop(LAG, CHIPS, both, (code, digits(TAKE)))[1]
    code = lax.fori_loop(CHIPS - LAG, CHIPS - 1, spread, code)
    spread(CHIPS - 1, code, True)

    for p in range(4):
        def drain(i, code, p=p):
            to = flipped(chip, lax.rem(code, 8))
            for b in range(2):
                @pl.when(to * 2 + b != me)
                def _():
                    sending(p, i, b, to).wait_send()
            return lax.div(code, 8)

        lax.fori_loop(0, CHIPS, drain, digits((SEND + [TAKE])[p]))


def solution(mesh):
    def step(x, gain, wq, wk, wv, wo):
        vmem, hbm = pl.BlockSpec(memory_space=pltpu.VMEM), pl.BlockSpec(memory_space=pltpu.HBM)
        bf16, f32 = jnp.bfloat16, jnp.float32
        return pl.pallas_call(
            kernel,
            out_shape=jax.ShapeDtypeStruct((OWN, DIM), bf16),
            in_specs=[hbm] * 6,
            out_specs=vmem,
            scratch_shapes=[
                pltpu.VMEM((OWN, DIM), bf16),
                pltpu.VMEM((DIM,), bf16),
                pltpu.VMEM((OWN, DIM), bf16),
                pltpu.VMEM((OWN, HEAD // 2), f32),
                pltpu.VMEM((OWN, HEAD // 2), f32),
                pltpu.VMEM((AHEAD + 1, DIM, PAIR), bf16),
                pltpu.VMEM((3 * CHIPS, 2, OWN, HEAD), bf16),
                pltpu.VMEM((CHIPS, PAIR, HEAD), bf16),
                pltpu.VMEM((CHIPS, HEAD + ONES, PAIR), bf16),
                pltpu.VMEM((CHIPS, PAIR, HEAD), bf16),
                pltpu.VMEM((CHIPS, PAIR, HEAD), bf16),
                pltpu.VMEM((OWN, DIM), bf16),
                pltpu.VMEM((1, PAIR), f32),
                pltpu.VMEM((HEAD + ONES, PAIR), f32),
                pltpu.VMEM((OWN, DIM), f32),
                pltpu.SemaphoreType.DMA((4,)),
                pltpu.SemaphoreType.DMA,
                pltpu.SemaphoreType.DMA((AHEAD + 1,)),
                pltpu.SemaphoreType.DMA((4, CHIPS, 2)),
                pltpu.SemaphoreType.DMA((4, CHIPS, 2)),
            ],
            compiler_params=pltpu.CompilerParams(collective_id=0, has_side_effects=True, vmem_limit_bytes=44 * 2**20),
            cost_estimate=pl.CostEstimate(flops=2 * OWN * DIM * DIM * 4 + 2 * 2 * 36 * PAIR * PAIR * HEAD, transcendentals=36 * PAIR * PAIR,
                                          bytes_accessed=4 * DIM * DIM * 2),
        )(*(pltpu.with_memory_space_constraint(t, pltpu.HBM) for t in (x, gain)), wq, wk, wv, wo)

    tokens, whole = P(("dp", "sp"), None), P(None, None)
    return jax.shard_map(
        step,
        mesh=mesh,
        in_specs=(tokens, P(None), whole, whole, whole, whole),
        out_specs=tokens,
        check_vma=False,
    )
```

```python
import functools
import math

import jax
import jax.numpy as jnp
from jax import lax
from jax.experimental import pallas as pl
from jax.experimental.pallas import tpu as pltpu
from jax.sharding import PartitionSpec as P

HEAD = 256
THETA = 10000
LOG2E = 1.4426950408889634
HIDDEN = -2e30
MESH = pl.DeviceIdType.MESH
OWN = 256
PAIR = 2 * HEAD
CHIPS = 8
DIM = 4096
ONES = 16
AHEAD = 2
TILE = PAIR
LAG = 5

LINKS = [7, 6, 1, 5, 2, 3, 4]
SEND = [LINKS + [0], LINKS + [0], [0] + LINKS]
TAKE = [0] + LINKS


def digits(values):
    return sum(v * 8**i for i, v in enumerate(values))


def flipped(n, mask):
    out = n
    for b in range(3):
        bit = lax.rem(lax.div(n, 2**b), 2)
        flip = lax.rem(lax.div(mask, 2**b), 2)
        out = out + flip * (1 - 2 * bit) * 2**b
    return out


def dot(a, b, ca, cb):
    return lax.dot_general(a, b, (((ca,), (cb,)), ((), ())), preferred_element_type=jnp.float32)


def kernel(x_hbm, gain_hbm, wq_hbm, wk_hbm, wv_hbm, wo_hbm, y_ref,
           x_ref, gain_ref, a_ref, cos_ref, sin_ref, w_ref, out_ref, keys, values, queries, seen_out, seen_in, top_s, mix_s, acc_ref,
           x_sem, gain_sem, w_sem, send_sem, recv_sem):
    me = lax.axis_index("sp")
    chip, core = lax.div(me, 2), lax.rem(me, 2)
    wide = [wk_hbm, wv_hbm, wq_hbm]

    def load_w(p, slot, other):
        return pltpu.make_async_copy(wide[p].at[:, pl.ds(pl.multiple_of(other * PAIR, PAIR), PAIR)], w_ref.at[slot], w_sem.at[slot])

    def load_wo(slot, other):
        for n in range(DIM // TILE):
            pltpu.make_async_copy(wo_hbm.at[pl.ds(pl.multiple_of(other * PAIR, PAIR), PAIR), pl.ds(n * TILE, TILE)],
                                  w_ref.at[slot, pl.ds(n * PAIR, PAIR), :], w_sem.at[slot]).start()

    def landing(p, c, b):
        at = pl.ds(pl.multiple_of(b * OWN, OWN), OWN)
        if p == 0:
            return keys.at[c, at, :]
        if p == 1:
            return values.at[c, pl.ds(0, HEAD), at]
        if p == 2:
            return queries.at[c, at, :]
        return seen_in.at[:, pl.ds(pl.multiple_of(c * PAIR + b * HEAD, HEAD), HEAD)]

    def part(p, i, b):
        if p < 3:
            return out_ref.at[p * CHIPS + i, b]
        return seen_out.at[i, pl.ds(b * OWN, OWN), :]

    def sending(p, i, b, to):
        return pltpu.make_async_remote_copy(
            src_ref=part(p, i, b), dst_ref=landing(p, chip, core), send_sem=send_sem.at[p, i, b],
            recv_sem=recv_sem.at[p, chip, core], device_id={"sp": to * 2 + b}, device_id_type=MESH)

    def send(p, i, to):
        for b in range(2):
            @pl.when(to * 2 + b != me)
            def _():
                sending(p, i, b, to).start()

            @pl.when(to * 2 + b == me)
            def _():
                landing(p, chip, core)[...] = part(p, i, b)[...]

    def arrived(p, c):
        for b in range(2):
            @pl.when(c * 2 + b != me)
            def _():
                pltpu.make_async_remote_copy(
                    src_ref=part(p, 0, b), dst_ref=landing(p, c, b), send_sem=send_sem.at[p, 0, b],
                    recv_sem=recv_sem.at[p, c, b], device_id={"sp": c * 2 + b}, device_id_type=MESH).wait_recv()

    x_copies = [pltpu.make_async_copy(x_hbm.at[pl.ds(n * 64, 64)], x_ref.at[pl.ds(n * 64, 64)], x_sem.at[n]) for n in range(4)]
    for x_copy in x_copies:
        x_copy.start()
    gain_copy = pltpu.make_async_copy(gain_hbm, gain_ref, gain_sem)
    gain_copy.start()
    load_w(0, 0, flipped(chip, SEND[0][0])).start()
    barrier = pltpu.get_barrier_semaphore()
    for n in range(1, 16):
        pl.semaphore_signal(barrier, inc=1, device_id={"sp": lax.rem(me + n, 16)}, device_id_type=MESH)

    half = HEAD // 2
    place = lax.broadcasted_iota(jnp.int32, (OWN, half), 0) + me * OWN
    power = lax.broadcasted_iota(jnp.int32, (1, half), 1).astype(jnp.float32) * (-math.log2(THETA) / half)
    angle = place.astype(jnp.float32) * jnp.exp2(power)
    cos_ref[...] = jnp.cos(angle)
    sin_ref[...] = jnp.sin(angle)
    values[:, HEAD:, :] = jnp.ones((CHIPS, ONES, PAIR), jnp.bfloat16)
    gain_copy.wait()

    def norm(r, _):
        rows = pl.ds(pl.multiple_of(r * 32, 32), 32)
        t = x_ref[rows, :].astype(jnp.float32)
        scale = lax.rsqrt(jnp.mean(t * t, -1, keepdims=True) + 1e-6)
        acc_ref[rows, :] = t
        a_ref[rows, :] = (t * scale * gain_ref[...].reshape(1, DIM).astype(jnp.float32)).astype(jnp.bfloat16)

    for n in range(4):
        x_copies[n].wait()
        lax.fori_loop(n * 2, n * 2 + 2, norm, None)
    load_w(0, 1, flipped(chip, SEND[0][1])).start()
    pl.semaphore_wait(barrier, 15)

    def turned(t):
        cos, sin = cos_ref[...], sin_ref[...]
        a, b = t[:, : HEAD // 2].astype(jnp.float32), t[:, HEAD // 2 :].astype(jnp.float32)
        return jnp.concatenate([a * cos - b * sin, b * cos + a * sin], -1).astype(jnp.bfloat16)

    for p in range(3):
        def project(i, code, p=p):
            t = p * CHIPS + i
            slot, later = lax.rem(t, AHEAD + 1), lax.rem(t + AHEAD, AHEAD + 1)
            other = flipped(chip, lax.rem(code, 8))
            after = flipped(chip, lax.rem(lax.div(code, 8**AHEAD), 8))

            @pl.when(i < CHIPS - AHEAD)
            def _():
                load_w(p, later, after).start()

            @pl.when(i >= CHIPS - AHEAD)
            def _():
                if p < 2:
                    load_w(p + 1, later, after).start()
                else:
                    load_wo(later, after)

            load_w(p, slot, other).wait()
            made = jnp.dot(a_ref[...], w_ref[slot], preferred_element_type=jnp.float32).astype(jnp.bfloat16)
            for b in range(2):
                one = made[:, b * HEAD : (b + 1) * HEAD]
                out_ref[t, b] = one.T if p == 1 else turned(one)
            send(p, i, other)
            return lax.div(code, 8)

        lax.fori_loop(0, CHIPS, project, digits(SEND[p] + (SEND + [TAKE])[p + 1][:AHEAD]))

    lax.fori_loop(0, CHIPS, lambda c, _: (arrived(0, c), arrived(1, c), None)[-1], None)

    e = HEAD**-0.5 * LOG2E

    def unit(c, blocks, first=False):
        q = queries[c]
        strips = [(s, slice(s * 256, (s + 1) * 256)) for s in range(2)]
        scores = [[dot(keys[j], q[at, :], 1, 1) for j in blocks] for _, at in strips]
        for (s, at), score in zip(strips, scores):
            if first:
                key = lax.broadcasted_iota(jnp.int32, score[0].shape, 0)
                query = lax.broadcasted_iota(jnp.int32, score[0].shape, 1) + s * 256
                score = [jnp.where(key <= query, score[0], HIDDEN)]
            top = functools.reduce(jnp.maximum, [t.max(axis=0, keepdims=True) for t in score])
            if not first:
                old = top_s[:, at]
                top = jnp.maximum(old, top)
            top_s[:, at] = top
            weights = [jnp.exp2((t - top) * e).astype(jnp.bfloat16) for t in score]
            mix = sum(dot(values[j], w, 1, 0) for j, w in zip(blocks, weights))
            mix_s[:, at] = mix if first else mix_s[:, at] * jnp.exp2((old - top) * e) + mix

    def attend(i, code):
        c = flipped(chip, lax.rem(code, 8))
        arrived(2, c)
        unit(c, (c,), True)
        lax.fori_loop(0, lax.div(c, 2), lambda j, _: unit(c, (2 * j, 2 * j + 1)), None)

        @pl.when(lax.rem(c, 2) == 1)
        def _():
            unit(c, (c - 1,))

        got = mix_s[:HEAD, :] * (1 / mix_s[HEAD : HEAD + 1, :])
        seen_out[i] = got.astype(jnp.bfloat16).T
        send(3, i, c)
        return lax.div(code, 8)

    def spread(i, code, last=False):
        t = 3 * CHIPS + i
        slot, later = lax.rem(t, AHEAD + 1), lax.rem(t + AHEAD, AHEAD + 1)
        other = flipped(chip, lax.rem(code, 8))
        after = flipped(chip, lax.rem(lax.div(code, 8**AHEAD), 8))

        @pl.when(i < CHIPS - AHEAD)
        def _():
            load_wo(later, after)

        load_w(0, slot, other).wait()
        arrived(3, other)
        left = seen_in[:, pl.ds(pl.multiple_of(other * PAIR, PAIR), PAIR)]
        for n in range(DIM // TILE):
            at = slice(n * TILE, (n + 1) * TILE)
            total = acc_ref[:, at] + jnp.dot(left, w_ref[slot, n * PAIR : (n + 1) * PAIR, :], preferred_element_type=jnp.float32)
            if last:
                y_ref[:, at] = total.astype(jnp.bfloat16)
            else:
                acc_ref[:, at] = total
        return lax.div(code, 8)

    def both(i, codes):
        return attend(i, codes[0]), spread(i - LAG, codes[1])

    code = lax.fori_loop(0, LAG, attend, digits(TAKE))
    code = lax.fori_loop(LAG, CHIPS, both, (code, digits(TAKE)))[1]
    code = lax.fori_loop(CHIPS - LAG, CHIPS - 1, spread, code)
    spread(CHIPS - 1, code, True)

    for p in range(4):
        def drain(i, code, p=p):
            to = flipped(chip, lax.rem(code, 8))
            for b in range(2):
                @pl.when(to * 2 + b != me)
                def _():
                    sending(p, i, b, to).wait_send()
            return lax.div(code, 8)

        lax.fori_loop(0, CHIPS, drain, digits((SEND + [TAKE])[p]))


def solution(mesh):
    def step(x, gain, wq, wk, wv, wo):
        vmem, hbm = pl.BlockSpec(memory_space=pltpu.VMEM), pl.BlockSpec(memory_space=pltpu.HBM)
        bf16, f32 = jnp.bfloat16, jnp.float32
        return pl.pallas_call(
            kernel,
            out_shape=jax.ShapeDtypeStruct((OWN, DIM), bf16),
            in_specs=[hbm] * 6,
            out_specs=vmem,
            scratch_shapes=[
                pltpu.VMEM((OWN, DIM), bf16),
                pltpu.VMEM((DIM,), bf16),
                pltpu.VMEM((OWN, DIM), bf16),
                pltpu.VMEM((OWN, HEAD // 2), f32),
                pltpu.VMEM((OWN, HEAD // 2), f32),
                pltpu.VMEM((AHEAD + 1, DIM, PAIR), bf16),
                pltpu.VMEM((3 * CHIPS, 2, OWN, HEAD), bf16),
                pltpu.VMEM((CHIPS, PAIR, HEAD), bf16),
                pltpu.VMEM((CHIPS, HEAD + ONES, PAIR), bf16),
                pltpu.VMEM((CHIPS, PAIR, HEAD), bf16),
                pltpu.VMEM((CHIPS, PAIR, HEAD), bf16),
                pltpu.VMEM((OWN, DIM), bf16),
                pltpu.VMEM((1, PAIR), f32),
                pltpu.VMEM((HEAD + ONES, PAIR), f32),
                pltpu.VMEM((OWN, DIM), f32),
                pltpu.SemaphoreType.DMA((4,)),
                pltpu.SemaphoreType.DMA,
                pltpu.SemaphoreType.DMA((AHEAD + 1,)),
                pltpu.SemaphoreType.DMA((4, CHIPS, 2)),
                pltpu.SemaphoreType.DMA((4, CHIPS, 2)),
            ],
            compiler_params=pltpu.CompilerParams(collective_id=0, has_side_effects=True, vmem_limit_bytes=44 * 2**20),
            cost_estimate=pl.CostEstimate(flops=2 * OWN * DIM * DIM * 4 + 2 * 2 * 36 * PAIR * PAIR * HEAD, transcendentals=36 * PAIR * PAIR,
                                          bytes_accessed=4 * DIM * DIM * 2),
        )(*(pltpu.with_memory_space_constraint(t, pltpu.HBM) for t in (x, gain)), wq, wk, wv, wo)

    tokens, whole = P(("dp", "sp"), None), P(None, None)
    return jax.shard_map(
        step,
        mesh=mesh,
        in_specs=(tokens, P(None), whole, whole, whole, whole),
        out_specs=tokens,
        check_vma=False,
    )
```
